64 devices in a mesh: dp: 4 (over x, y), sp: 16 (over z, core).
Axes of the slice: x: 2, y: 2, z: 8, core: 2. Of those that a mesh axis runs over, the one named last changes fastest.
The devices are a block of a 4x4x8 slice.
Arguments:
- latent: bfloat16 [32, 128, 128, 4], P('dp', 'sp'), parts along dimension 0
- time_emb: bfloat16 [32, 1536], P('dp'), parts along dimension 0
- w_in: bfloat16 [3, 3, 4, 384], replicated
- b_in: bfloat16 [384], replicated
- gn1_scale: bfloat16 [2, 384], replicated
- gn1_shift: bfloat16 [2, 384], replicated
- conv1_w: bfloat16 [2, 3, 3, 384, 384], replicated
- conv1_b: bfloat16 [2, 384], replicated
- temb_w: bfloat16 [2, 1536, 384], replicated
- temb_b: bfloat16 [2, 384], replicated
- gn2_scale: bfloat16 [2, 384], replicated
- gn2_shift: bfloat16 [2, 384], replicated
- conv2_w: bfloat16 [2, 3, 3, 384, 384], replicated
- conv2_b: bfloat16 [2, 384], replicated
- down_w: bfloat16 [3, 3, 384, 384], replicated
- down_b: bfloat16 [384], replicated
Outputs:
- output 1: bfloat16 [32, 128, 128, 384], P('dp', 'sp'), parts along dimension 0
- output 2: bfloat16 [32, 128, 128, 384], P('dp', 'sp'), parts along dimension 0
- output 3: bfloat16 [32, 128, 128, 384], P('dp', 'sp'), parts along dimension 0
- output 4: bfloat16 [32, 64, 64, 384], P('dp', 'sp'), parts along dimension 0
There are 4 independent parts. The reference program is written for one: setup_inputs(seed, part) draws one part's arguments, and reference() takes and returns one part's arrays. A program takes and returns all parts, laid end to end along the dimension named above; an argument that names none is the same for every part.
All inputs are finite; a program needn't handle non-finite values.
Results may differ from the reference program's by a relative error of at most 0.0133381.
Values are sent between devices in bfloat16 or wider.
A program may use at most 768 MiB of HBM per device.

```python
import jax
import jax.numpy as jnp
from jax import lax

BATCH = 8
HEIGHT = 128
WIDTH = 128
CHANNELS = 384
TEMB_DIM = 1536
LATENT_CH = 4
GROUPS = 32
LAYERS = 2
GN_EPS = 1e-5


def setup_inputs(seed: int = 0, part: int = 0) -> dict:
    part_keys = jax.random.split(jax.random.fold_in(jax.random.key(seed), part), 4)
    shared_keys = jax.random.split(jax.random.key(seed + 1), 14)
    row_pos = jnp.linspace(-1.0, 1.0, HEIGHT)[None, :, None, None]
    noise_part = jax.random.normal(part_keys[0], (BATCH, HEIGHT, WIDTH, LATENT_CH), jnp.float32)
    row_slope = 1.5 * jax.random.normal(part_keys[1], (BATCH, 1, 1, LATENT_CH), jnp.float32)
    row_curve = jax.random.normal(part_keys[2], (BATCH, 1, 1, LATENT_CH), jnp.float32)
    latent = noise_part + row_slope * row_pos + row_curve * (1.5 * row_pos * row_pos - 0.5)
    time_emb = jax.random.normal(part_keys[3], (BATCH, TEMB_DIM), jnp.float32)
    conv_std = 1.2 * (9 * CHANNELS) ** -0.5

    def draw_w(key_slot, arr_shape, spread, center):
        return (center + spread * jax.random.normal(shared_keys[key_slot], arr_shape, jnp.float32)).astype(jnp.bfloat16)

    return {
        "latent": latent.astype(jnp.bfloat16),
        "time_emb": time_emb.astype(jnp.bfloat16),
        "w_in": draw_w(0, (3, 3, LATENT_CH, CHANNELS), (9 * LATENT_CH) ** -0.5, 0.0),
        "b_in": draw_w(1, (CHANNELS,), 0.5, 0.0),
        "gn1_scale": draw_w(2, (LAYERS, CHANNELS), 0.3, 1.0),
        "gn1_shift": draw_w(3, (LAYERS, CHANNELS), 0.3, 0.0),
        "conv1_w": draw_w(4, (LAYERS, 3, 3, CHANNELS, CHANNELS), conv_std, 0.0),
        "conv1_b": draw_w(5, (LAYERS, CHANNELS), 0.3, 0.0),
        "temb_w": draw_w(6, (LAYERS, TEMB_DIM, CHANNELS), TEMB_DIM ** -0.5, 0.0),
        "temb_b": draw_w(7, (LAYERS, CHANNELS), 0.3, 0.0),
        "gn2_scale": draw_w(8, (LAYERS, CHANNELS), 0.3, 1.0),
        "gn2_shift": draw_w(9, (LAYERS, CHANNELS), 0.3, 0.0),
        "conv2_w": draw_w(10, (LAYERS, 3, 3, CHANNELS, CHANNELS), conv_std, 0.0),
        "conv2_b": draw_w(11, (LAYERS, CHANNELS), 0.3, 0.0),
        "down_w": draw_w(12, (3, 3, CHANNELS, CHANNELS), (9 * CHANNELS) ** -0.5, 0.0),
        "down_b": draw_w(13, (CHANNELS,), 0.3, 0.0),
    }


def conv_same(inputs, kernel, bias_c, stride):
    out_f32 = lax.conv_general_dilated(inputs[None].astype(jnp.float32), kernel.astype(jnp.float32), (stride, stride), ((1, 1), (1, 1)), dimension_numbers=("NHWC", "HWIO", "NHWC"))
    return (out_f32[0] + bias_c.astype(jnp.float32)).astype(jnp.bfloat16)


def norm_silu(values, gain_c, shift_c):
    grouped = values.reshape(values.shape[0] * values.shape[1], GROUPS, CHANNELS // GROUPS)
    grp_mean = jnp.mean(grouped, axis=(0, 2), keepdims=True)
    grp_var = jnp.mean(jnp.square(grouped - grp_mean), axis=(0, 2), keepdims=True)
    normed = ((grouped - grp_mean) * lax.rsqrt(grp_var + GN_EPS)).reshape(values.shape)
    normed = normed * gain_c.astype(jnp.float32) + shift_c.astype(jnp.float32)
    return jax.nn.silu(normed).astype(jnp.bfloat16)


def reference(latent, time_emb, w_in, b_in, gn1_scale, gn1_shift, conv1_w, conv1_b, temb_w, temb_b, gn2_scale, gn2_shift, conv2_w, conv2_b, down_w, down_b):
    layer_params = (gn1_scale, gn1_shift, conv1_w, conv1_b, temb_w, temb_b, gn2_scale, gn2_shift, conv2_w, conv2_b)

    def one_sample(sample):
        latent_s, temb_s = sample
        first_out = conv_same(latent_s, w_in, b_in, 1)
        emb_act = jax.nn.silu(temb_s.astype(jnp.float32)).astype(jnp.bfloat16)

        def layer_step(hidden, params):
            norm_g1, norm_b1, conv_w1, conv_b1, proj_w, proj_b, norm_g2, norm_b2, conv_w2, conv_b2 = params
            branch = conv_same(norm_silu(hidden.astype(jnp.float32), norm_g1, norm_b1), conv_w1, conv_b1, 1)
            emb_proj = jnp.dot(emb_act.astype(jnp.float32), proj_w.astype(jnp.float32)) + proj_b.astype(jnp.float32)
            mixed_in = branch.astype(jnp.float32) + emb_proj
            branch = conv_same(norm_silu(mixed_in, norm_g2, norm_b2), conv_w2, conv_b2, 1)
            hidden = (hidden.astype(jnp.float32) + branch.astype(jnp.float32)).astype(jnp.bfloat16)
            return hidden, hidden

        last_out, per_layer = lax.scan(layer_step, first_out, layer_params)
        return first_out, per_layer, conv_same(last_out, down_w, down_b, 2)

    firsts, layers_out, down_outs = lax.map(one_sample, (latent, time_emb))
    return firsts, layers_out[:, 0], layers_out[:, 1], down_outs
```

```python
import functools

import jax
import jax.numpy as jnp
from jax import lax
from jax.experimental import pallas as pl
from jax.experimental.pallas import tpu as pltpu
from jax.sharding import PartitionSpec as P

GN_GROUPS = 32
GN_EPS = 1e-5
MESH = pl.DeviceIdType.MESH
F32 = jnp.float32
BF16 = jnp.bfloat16
MCHUNK = 512
BUSY = 3


def exact_dot(rows, select):
    k = rows.shape[0]
    high = rows.astype(BF16).astype(F32)
    rest = rows - high
    mid = rest.astype(BF16).astype(F32)
    parts = [high, mid, rest - mid]
    if 3 * k < 16:
        parts.append(jnp.zeros((16 - 3 * k, rows.shape[1]), F32))
    out = jnp.dot(jnp.concatenate(parts, axis=0).astype(BF16), select, preferred_element_type=F32)
    return out[:k] + out[k:2 * k] + out[2 * k:3 * k]


def weight_copies(src, to_a, to_b, ch, last):
    n_a, lanes = to_a.shape[0], to_a.shape[-1]
    wide = n_a * lanes
    cps = [(src.at[:, :, :, pl.ds(k * lanes, lanes)], to_a.at[k]) for k in range(n_a)]
    cps.append((src.at[:, 1, :, pl.ds(wide, lanes)], to_b.at[0, :, pl.ds(0, ch)]))
    cps.append((src.at[:, 2, :, pl.ds(wide, lanes)], to_b.at[0, :, pl.ds(ch, ch)]))
    cps.append((src.at[:, 0, :, pl.ds(wide, lanes)], to_b.at[1, :, pl.ds(ch if last else 0, ch)]))
    return cps


def down_blocks(ch, lanes):
    wide = ch - lanes
    taps = [(dy, dx) for dy in range(3) for dx in range(3)]
    blocks = [(dy, dx, c) for c in range(0, wide, lanes) for dy, dx in taps]
    blocks += [(dy, dx, wide) for dy in range(3) for dx in (1, 2)]
    return blocks + [(dy, 0, wide) for dy in range(3)]


def block_at(hu, b, first, ch):
    n_tiles = hu.shape[1]
    return hu.at[first + b // (2 * n_tiles), b // 2 % n_tiles, pl.ds(b % 2 * ch, ch)]


def mix(a, b):
    both = [((k + 1) / (len(a) + 1), f) for k, f in enumerate(a)] + [((k + 1) / (len(b) + 1), f) for k, f in enumerate(b)]
    return [f for _, f in sorted(both, key=lambda t: t[0])]


def kernel(n, group, lat, temb, w_in, b_in, gn1_scale, gn1_shift, b1, temb_b, gn2_scale, gn2_shift, b2, temb_w, w1, w2, wd, down_b,
           hu, x0, x1, wa, wb, halo, gstat, lat_v, shift, in_w, vecs, emb, gather, spread, held, t_sem, w_sem, lat_sem, halo_sem, stat_sem, send_sem, stat_send, lat_send, edge_sem, edge_send, down_sem):
    n_tiles, n_pos, lanes = hu.shape[1:]
    n_batch = halo.shape[1]
    ch = n_tiles * lanes
    cols = halo.shape[4]
    rows = n_pos // cols
    n_layer = w1.shape[0]
    me = lax.axis_index("sp")
    nxt = lax.rem(me + 1, n)
    prv = lax.rem(me + n - 1, n)
    n_slots = wa.shape[0]
    wide = wa.shape[1] * lanes

    def wcopies(p):
        cps = weight_copies((w1, w2)[p % 2].at[p // 2], wa.at[p % wa.shape[0]], wb.at[p % wa.shape[0]], ch, False)
        return [pltpu.make_async_copy(a, b, w_sem.at[p, k]) for k, (a, b) in enumerate(cps)]

    lat_local = pltpu.make_async_copy(lat, lat_v.at[:, pl.ds(1, rows)], lat_sem.at[2])
    lat_local.start()
    t_rows = temb_w.shape[1]
    t_parts = [(l, lo, min(n_pos, t_rows - lo)) for l in range(n_layer) for lo in range(0, t_rows, n_pos)]

    def temb_slot(j):
        return (n_layer + 1) * n_batch + j

    temb_copies = [pltpu.make_async_copy(temb_w.at[l, pl.ds(lo, size), pl.ds(k * lanes, lanes)], hu.at[temb_slot(j), k, pl.ds(0, size)], t_sem.at[j, k]) for j, (l, lo, size) in enumerate(t_parts) for k in range(n_tiles)]
    for cp in temb_copies:
        cp.start()
    for cp in wcopies(0):
        cp.start()

    barrier = pltpu.get_barrier_semaphore()
    for k in range(1, n):
        pl.semaphore_signal(barrier, inc=1, device_id={"sp": lax.rem(me + k, n)}, device_id_type=MESH)
    lat_local.wait()
    pl.semaphore_wait(barrier, n - 1)

    lat_down = pltpu.make_async_remote_copy(lat_v.at[:, rows], lat_v.at[:, 0], lat_send.at[0], lat_sem.at[0], device_id={"sp": nxt}, device_id_type=MESH)
    lat_up = pltpu.make_async_remote_copy(lat_v.at[:, 1], lat_v.at[:, rows + 1], lat_send.at[1], lat_sem.at[1], device_id={"sp": prv}, device_id_type=MESH)
    lat_down.start()
    lat_up.start()
    for p in range(1, n_slots):
        for cp in wcopies(p):
            cp.start()
    for p in range(n_slots):
        wb[p, 1, :, pl.ds(ch, ch)] = jnp.zeros((3, ch, lanes), BF16)

    blank = jnp.zeros((4, ch), F32)
    in_w[...] = jnp.concatenate([w_in[dy, dx].astype(F32) if dx < 3 else blank for dy in range(3) for dx in range(4)], axis=0).astype(BF16)
    zrow = jnp.zeros((1, ch), F32)
    for p in range(2 * n_layer + 1):
        if p == 2 * n_layer:
            table = [zrow, zrow, zrow]
        else:
            refs = ((gn1_scale, gn1_shift, b1), (gn2_scale, gn2_shift, b2))[p % 2]
            table = [ref[pl.ds(p // 2, 1)].astype(F32) for ref in refs]
        vecs[p] = jnp.concatenate(table + [zrow] * 5, axis=0)
    lanes_of = lax.broadcasted_iota(jnp.int32, (ch, 128), 0) - group * lax.rem(lax.broadcasted_iota(jnp.int32, (ch, 128), 1), GN_GROUPS)
    gather[...] = jnp.where(jnp.logical_and(lanes_of >= 0, lanes_of < group), 1.0, 0.0).astype(BF16)
    lanes_of = lax.broadcasted_iota(jnp.int32, (128, ch), 1) - group * lax.rem(lax.broadcasted_iota(jnp.int32, (128, ch), 0), GN_GROUPS)
    spread[...] = jnp.where(jnp.logical_and(lanes_of >= 0, lanes_of < group), 1.0, 0.0).astype(BF16)
    for cp in temb_copies:
        cp.wait()
    z = temb[...].astype(F32) * 0.5
    act = (z + z * jnp.tanh(z)).astype(BF16)
    for p in range(2 * n_layer + 1):
        if p % 2:
            total = temb_b[pl.ds(p // 2, 1)].astype(F32)
            for j, (l, lo, size) in enumerate(t_parts):
                if l == p // 2:
                    part = jnp.concatenate([hu[temb_slot(j), k, pl.ds(0, size)] for k in range(n_tiles)], axis=1)
                    total = total + jnp.dot(act[:, lo:lo + size], part, preferred_element_type=F32)
            emb[p] = total
        else:
            emb[p] = jnp.zeros((n_batch, ch), F32)

    def weights_a(p):
        return jnp.concatenate([wa[lax.rem(p, n_slots), k].reshape(9 * ch, lanes) for k in range(wide // lanes)], axis=1)

    def weights_b(p):
        return jnp.concatenate([wb[lax.rem(p, n_slots), k].reshape(6 * ch, lanes) for k in range(2)], axis=1)

    def source(p):
        odd = lax.rem(p, 2)
        return ((1 - odd) * (p // 2) + odd * (n_layer + 1)) * n_batch

    def edge_down(s):
        return pltpu.make_async_remote_copy(hu.at[n_layer * n_batch + s, :, pl.ds(n_pos - cols, cols)], hu.at[(n_layer + 2) * n_batch, :, pl.ds(s * cols, cols)], edge_send.at[s], edge_sem.at[s], device_id={"sp": nxt}, device_id_type=MESH)

    def halo_down(p, s):
        buf = source(p)
        return pltpu.make_async_remote_copy(hu.at[buf + s, :, pl.ds(n_pos - cols, cols)], halo.at[p, s, 0], send_sem.at[p, s, 0], halo_sem.at[p, s, 0], device_id={"sp": nxt}, device_id_type=MESH)

    def halo_up(p, s):
        buf = source(p)
        return pltpu.make_async_remote_copy(hu.at[buf + s, :, pl.ds(0, cols)], halo.at[p, s, 1], send_sem.at[p, s, 1], halo_sem.at[p, s, 1], device_id={"sp": prv}, device_id_type=MESH)

    def stat_copy(p, i, k):
        return pltpu.make_async_remote_copy(gstat.at[p, i, 0], gstat.at[p, i, k], stat_send.at[p, i], stat_sem.at[p, i], device_id={"sp": lax.rem(me + k, n)}, device_id_type=MESH)

    def stat_all(p, i):
        return pltpu.make_async_remote_copy(gstat.at[p, i, pl.ds(1, n - 1)], gstat.at[p, i, pl.ds(1, n - 1)], stat_send.at[p, i], stat_sem.at[p, i], device_id={"sp": nxt}, device_id_type=MESH)

    def send_stats(p, i):
        for k in range(1, n):
            stat_copy(p, i, k).start()

    def send_rows(p, i):
        for s in (2 * i, 2 * i + 1):
            halo_down(p, s).start()
            halo_up(p, s).start()

    own_lanes = lax.broadcasted_iota(jnp.int32, (4, 128), 1) - GN_GROUPS * lax.broadcasted_iota(jnp.int32, (4, 128), 0)
    own_lanes = jnp.logical_and(own_lanes >= 0, own_lanes < GN_GROUPS)

    def keep_sums(q, sums):
        held[q] = jnp.concatenate(sums + [jnp.zeros((4, ch), F32)], axis=0)

    def put_stats(p, i, q):
        tot = exact_dot(held[q][:4], gather[...])
        gstat[p, i, 0] = jnp.sum(jnp.where(own_lanes, tot, 0.0), axis=0, keepdims=True)

    def arrive_rows(p, s):
        halo_down(p, s).wait_recv()
        halo_up(p, s).wait_recv()

    def coefficients(p, s, which):
        tot = jnp.sum(gstat[p, s // 2], axis=0)
        pick = own_lanes[2 * which:2 * which + 2]
        tot = exact_dot(jnp.where(pick, tot, 0.0), spread[...])
        count = float(n * n_pos * group)
        mean = tot[0:1] / count
        var = tot[1:2] / count - mean * mean
        v = vecs[p]
        scale = lax.rsqrt(var + GN_EPS) * v[0:1]
        offset = v[1:2] - mean * scale + emb[p, pl.ds(s, 1)] * scale
        return scale * 0.5, offset * 0.5

    pad = 8
    shift[...] = jnp.zeros_like(shift)

    def norm_piece(p, s, r, k, scale, offset, x):
        scale, offset = scale[:, k * 128:(k + 1) * 128], offset[:, k * 128:(k + 1) * 128]
        if r == 0:
            src = halo[p, s, 0, k]
            keep = (me > 0).astype(F32)
            scale, offset = scale * keep, offset * keep
        elif r == rows + 1:
            src = halo[p, s, 1, k]
            keep = (me < n - 1).astype(F32)
            scale, offset = scale * keep, offset * keep
        else:
            src = hu[source(p) + s, k, pl.ds((r - 1) * cols, cols)]
        z = src.astype(F32) * scale + offset
        y = z + z * jnp.tanh(z)
        at = pl.ds(r * cols, cols)
        slot = (r * n_tiles + k) % shift.shape[0]
        shift[slot, pl.ds(pad, cols)] = y
        x[n_tiles + k, at] = y.astype(BF16)
        x[k, at] = shift[slot, pl.ds(pad - 1, cols)].astype(BF16)
        x[2 * n_tiles + k, at] = shift[slot, pl.ds(pad + 1, cols)].astype(BF16)

    def norm_work(p, s, which, x):
        coef = []

        def first():
            coef.extend(coefficients(p, s, which))

        def piece(r, k):
            return lambda: norm_piece(p, s, r, k, coef[0], coef[1], x)

        return [first] + [piece(r, k) for r in range(rows + 2) for k in range(ch // 128)]

    def conv_sample(p, s, x, side):
        odd = lax.rem(p, 2)
        bias = vecs[p, 2:3]
        e_next = emb[p + 1, pl.ds(s, 1)]
        tail = ch - wide
        col0 = lax.broadcasted_iota(jnp.int32, (cols, tail), 0) == 0
        sums_a = [(jnp.zeros((8, wide), F32),) * 2]
        sums_b = [(jnp.zeros((8, tail), F32),) * 2]

        def finish(at, lo, width, raw, sums):
            parts = []
            for k in range(lo // 128, (lo + width) // 128):
                piece = slice(k * 128, (k + 1) * 128)
                out = (raw[:, k * 128 - lo:(k + 1) * 128 - lo] + bias[:, piece]).astype(BF16).astype(F32)
                old = hu[p // 2 * n_batch + s, k, at].astype(F32)
                new = (jnp.where(odd == 1, old, 0.0) + out).astype(BF16)
                hu[source(p + 1) + s, k, at] = new
                v = new.astype(F32) + e_next[:, piece]
                v = v.reshape(v.shape[0] // 8, 8, 128)
                parts.append((jnp.sum(v, axis=0), jnp.sum(v * v, axis=0)))
            sums[0] = tuple(old + jnp.concatenate([q[j] for q in parts], axis=1) for j, old in enumerate(sums[0]))

        def end_a(m, j, a):
            return lambda: finish(pl.ds(m + j * cols, cols), 0, wide, a[j * cols:(j + 1) * cols], sums_a)

        def end_b(m, j, b):
            def work():
                part = b[j * cols:(j + 1) * cols]
                raw = part[:, :tail] + jnp.where(col0, 0.0, pltpu.roll(part[:, tail:], 1, axis=0))
                finish(pl.ds(m + j * cols, cols), wide, tail, raw, sums_b)
            return work

        n_dots = 2 * (n_pos // MCHUNK)
        side = list(side)
        share = -(-len(side) // min(BUSY, n_dots))
        pending = []
        for m in range(0, n_pos, MCHUNK):
            for kind in range(2):
                lo = ch if kind else 0
                lhs = jnp.concatenate([x[k, pl.ds(m + dy * cols, MCHUNK)] for dy in range(3) for k in range(lo // 128, 3 * n_tiles)], axis=1)
                w = weights_b(p) if kind else weights_a(p)
                out = jnp.dot(lhs, w, preferred_element_type=F32)
                now, side = side[:share], side[share:]
                for f in mix(pending, now):
                    f()
                pending = [(end_b if kind else end_a)(m, j, out) for j in range(MCHUNK // cols)]
        for f in pending:
            f()
        return [jnp.concatenate([jnp.sum(sa, axis=0, keepdims=True), jnp.sum(sb, axis=0, keepdims=True)], axis=1) for sa, sb in zip(sums_a[0], sums_b[0])]

    lat_down.wait_recv()
    lat_up.wait_recv()

    half = n_batch // 2

    def conv_in(s):
        tiles = []
        for r in range(rows + 2):
            t = lat_v[s, r]
            if r == 0:
                t = jnp.where(me > 0, t, jnp.zeros_like(t))
            if r == rows + 1:
                t = jnp.where(me < n - 1, t, jnp.zeros_like(t))
            tiles.append(t)
        lhs = jnp.concatenate([jnp.concatenate(tiles[r:r + 3], axis=0) for r in range(rows)], axis=1)
        out = lax.dot_general(lhs, in_w[...], (((0,), (0,)), ((), ())), preferred_element_type=F32)
        new = (out + b_in[...].astype(F32).reshape(1, ch)).astype(BF16)
        for k in range(n_tiles):
            hu[s, k] = new[:, k * 128:(k + 1) * 128]
        v = new.astype(F32)
        return [jnp.sum(v, axis=0, keepdims=True), jnp.sum(v * v, axis=0, keepdims=True)]

    def conv_in_step(i, carry):
        @pl.when(i > 0)
        def _():
            send_stats(0, i - 1)
            send_rows(0, i - 1)

        keep_sums(i // (half - 1), conv_in(2 * i) + conv_in(2 * i + 1))
        put_stats(0, i, 0)
        return carry

    lax.fori_loop(0, half, conv_in_step, 0)
    send_rows(0, half - 1)
    stat_all(0, 0).wait_recv()
    arrive_rows(0, 0)
    for f in norm_work(0, 0, 0, x0):
        f()


    spare = (n_layer + 1) * n_batch
    down_list = down_blocks(ch, lanes)
    n_lent = len(down_list) // (2 * n_tiles) + 1
    down_copies = [pltpu.make_async_copy(wd.at[dy, dx, :, pl.ds(c, lanes)], block_at(hu, b, spare, ch), down_sem.at[b]) for b, (dy, dx, c) in enumerate(down_list)]

    def step(t, carry):
        p, i = t // half, lax.rem(t, half)
        s0, s1 = 2 * i, 2 * i + 1
        after = lax.rem(t + 1, half * 2 * n_layer)
        pn, sn = after // half, 2 * lax.rem(after, half)
        pb, ib = (t + half - 1) // half - 1, lax.rem(t + half - 1, half)
        ps, js = (t + half - 2) // half - 1, lax.rem(t + half - 2, half)
        arrive_rows(p, s1)

        @pl.when(t + 1 < half * 2 * n_layer)
        def _():
            stat_all(pn, sn // 2).wait_recv()
            arrive_rows(pn, sn)

        for q in range(2 * n_layer):
            @pl.when(jnp.logical_and(p == q, i == 0))
            def _():
                for cp in wcopies(q):
                    cp.wait()

        @pl.when(t == half * 2 * n_layer - 1)
        def _():
            for s in range(n_lent):
                halo_down(2 * n_layer - 1, s).wait_send()
                halo_up(2 * n_layer - 1, s).wait_send()
            for cp in down_copies:
                cp.start()

        for q in range(n_slots, 2 * n_layer):
            @pl.when(jnp.logical_and(p == q - n_slots + 1, i == 0))
            def _():
                for cp in wcopies(q):
                    cp.start()

        @pl.when(p > 0)
        def _():
            for s in (s0, s1):
                halo_down(p - 1, s).wait_send()
                halo_up(p - 1, s).wait_send()

        @pl.when(jnp.logical_and(t > 0, pb < 2 * n_layer - 1))
        def _():
            send_rows(pb + 1, ib)

        @pl.when(jnp.logical_and(t > 0, pb == 2 * n_layer - 1))
        def _():
            for j in range(2):
                edge_down(2 * ib + j).start()

        @pl.when(jnp.logical_and(t > 0, ps < 2 * n_layer - 1))
        def _():
            send_stats(ps + 1, js)

        old, new = lax.rem(t + 1, 2), lax.rem(t, 2)
        sums = conv_sample(p, s0, x0, [lambda: put_stats(pb + 1, ib, old)] + norm_work(p, s1, 1, x1))
        sums = sums + conv_sample(p, s1, x1, norm_work(pn, sn, 0, x0))
        keep_sums(new, sums)
        return carry

    lax.fori_loop(0, half * 2 * n_layer, step, 0)
    for j in range(2):
        edge_down(n_batch - 2 + j).start()
    bias_slot = spare + len(down_list) // (2 * n_tiles)
    bias_row = down_b[...].astype(F32).reshape(1, ch)
    for k in range(n_tiles):
        hu[bias_slot, k, pl.ds(n_pos - 16, 16)] = jnp.broadcast_to(bias_row[:, k * lanes:(k + 1) * lanes], (16, lanes)).astype(BF16)
    for cp in down_copies:
        cp.wait()

    def drain_stats(t, carry):
        stat_all(t // half, lax.rem(t, half)).wait_send()
        return carry

    lax.fori_loop(0, 2 * n_layer * half, drain_stats, 0)

    def drain_rows(s, carry):
        edge_down(s).wait()
        return carry

    for s in range(n_lent, n_batch):
        halo_down(2 * n_layer - 1, s).wait_send()
        halo_up(2 * n_layer - 1, s).wait_send()

    lax.fori_loop(0, n_batch, drain_rows, 0)
    lat_down.wait_send()
    lat_up.wait_send()


def down_kernel(hu, h0_out, h1_out, h2_out, d_out, x0, x1, shift, dn_out, out_sem, d_sem):
    n_tiles, n_pos, lanes = hu.shape[1:]
    n_batch, per, ch = d_out.shape
    cols = n_pos // n_batch
    rows = n_pos // cols
    me = lax.axis_index("sp")
    half = n_batch // 2
    pad = 8
    wide = ch - lanes
    spare = 3 * n_batch
    n_blocks = len(down_blocks(ch, lanes))
    blocks = [block_at(hu, b, spare, ch) for b in range(n_blocks)]
    outs = [pltpu.make_async_copy(hu.at[pl.ds(q * n_batch, n_batch), k], out.at[:, :, pl.ds(k * lanes, lanes)], out_sem.at[q, k]) for q, out in enumerate((h0_out, h1_out, h2_out)) for k in range(n_tiles)]
    for cp in outs:
        cp.start()
    shift[...] = jnp.zeros_like(shift)
    wide_out = cols // 2
    dn_rows = rows // 2
    per = dn_rows * wide_out

    def down_prep(s, base):
        for r in range(rows + 1):
            for k in range(n_tiles):
                if r == 0:
                    src = hu[hu.shape[0] - 1, k, pl.ds(s * cols, cols)].astype(F32) * (me > 0).astype(F32)
                else:
                    src = hu[2 * n_batch + s, k, pl.ds((r - 1) * cols, cols)].astype(F32)
                slot = (r * n_tiles + k) % shift.shape[0]
                shift[slot, pl.ds(pad, cols)] = src
                at = pl.ds(base + (r // 2) * wide_out, wide_out)
                x = x1 if r % 2 else x0
                for j in range(3):
                    x[j * n_tiles + k, at] = shift[slot, pl.ds(pad - 1 + j, wide_out, stride=2)].astype(BF16)

    def down_step(i, carry):
        stride = 512
        for j in range(2):
            down_prep(2 * i + j, j * stride)

        rest = 9 * (n_tiles - 1)
        w_a = jnp.concatenate([jnp.concatenate([blocks[c * 9 + k][...] for k in range(9)], axis=0) for c in range(n_tiles - 1)], axis=1)
        none = jnp.zeros((ch, lanes), BF16)
        w_here = jnp.concatenate([blocks[rest + k][...] for k in range(6)], axis=0)
        w_before = jnp.concatenate([v for k in range(3) for v in (none, blocks[rest + 6 + k][...])], axis=0)
        w_b = jnp.concatenate([w_here, w_before], axis=1)
        def lhs(lo):
            parts = []
            for x, off in ((x0, 0), (x1, 0), (x0, wide_out)):
                for k in range(lo // 128, 3 * n_tiles):
                    parts.append(jnp.concatenate([x[k, pl.ds(j * stride + off, per)] for j in range(2)], axis=0))
            return jnp.concatenate(parts, axis=1)

        bias = jnp.concatenate([hu[spare + n_blocks // (2 * n_tiles), k, pl.ds(n_pos - 16, 16)].astype(F32)[:1] for k in range(n_tiles)], axis=1)
        tail = ch - wide
        a = jnp.dot(lhs(0), w_a, preferred_element_type=F32)
        b = jnp.dot(lhs(ch), w_b, preferred_element_type=F32)
        edge = lax.rem(lax.broadcasted_iota(jnp.int32, (2 * per, tail), 0), wide_out) == 0
        b = b[:, :tail] + jnp.where(edge, 0.0, pltpu.roll(b[:, tail:], 1, axis=0))
        for j in range(2):
            dn_out[2 * i + j, :, pl.ds(0, wide)] = (a[j * per:(j + 1) * per] + bias[:, :wide]).astype(BF16)
            dn_out[2 * i + j, :, pl.ds(wide, tail)] = (b[j * per:(j + 1) * per] + bias[:, wide:]).astype(BF16)
        return carry

    lax.fori_loop(0, half, down_step, 0)
    last = pltpu.make_async_copy(dn_out, d_out, d_sem)
    last.start()
    for cp in outs:
        cp.wait()
    last.wait()


def solution(mesh):
    n = mesh.shape["sp"]

    def band_program(latent, time_emb, w_in, b_in, gn1_scale, gn1_shift, conv1_w, conv1_b, temb_w, temb_b, gn2_scale, gn2_shift, conv2_w, conv2_b, down_w, down_b):
        n_batch, rows, cols, lat_ch = latent.shape
        n_layer, ch = conv1_b.shape
        n_pos = rows * cols
        group = ch // GN_GROUPS
        wide = 256
        lt = jnp.transpose(latent, (0, 1, 3, 2))
        lp = jnp.pad(lt, ((0, 0), (0, 0), (0, 0), (1, 1)))
        shifted = [lp[..., k:k + cols] for k in range(3)]
        pad_rows = 16 - 3 * lat_ch
        lat = jnp.concatenate(shifted + [jnp.zeros((n_batch, rows, pad_rows, cols), BF16)], axis=2)
        any_spec = pl.BlockSpec(memory_space=pltpu.HBM)
        vmem = pl.BlockSpec(memory_space=pltpu.VMEM)
        full = jax.ShapeDtypeStruct((n_batch, n_pos, ch), BF16)
        per = n_pos // 4
        hu = pl.pallas_call(
            functools.partial(kernel, n, group),
            out_shape=pltpu.VMEM(((n_layer + 2) * n_batch + 1, ch // 128, n_pos, 128), BF16),
            in_specs=[any_spec] + [vmem] * 10 + [any_spec] * 4 + [vmem],
            out_specs=vmem,
            scratch_shapes=[
                pltpu.VMEM((3 * ch // 128, (rows + 2) * cols, 128), BF16),
                pltpu.VMEM((3 * ch // 128, (rows + 2) * cols, 128), BF16),
                pltpu.VMEM((3, wide // 128, 3, 3, ch, 128), BF16),
                pltpu.VMEM((3, 2, 3, 2 * ch, 128), BF16),
                pltpu.VMEM((2 * n_layer, n_batch, 2, ch // 128, cols, 128), BF16),
                pltpu.VMEM((2 * n_layer + 1, n_batch // 2, n, 1, 128), F32),
                pltpu.VMEM((n_batch, rows + 2, 16, cols), BF16),
                pltpu.VMEM((6, cols + 16, 128), F32),
                pltpu.VMEM((48, ch), BF16),
                pltpu.VMEM((2 * n_layer + 1, 8, ch), F32),
                pltpu.VMEM((2 * n_layer + 1, n_batch, ch), F32),
                pltpu.VMEM((ch, 128), BF16),
                pltpu.VMEM((128, ch), BF16),
                pltpu.VMEM((2, 8, ch), F32),
                pltpu.SemaphoreType.DMA((8, ch // 128)),
                pltpu.SemaphoreType.DMA((2 * n_layer, 5)),
                pltpu.SemaphoreType.DMA((3,)),
                pltpu.SemaphoreType.DMA((2 * n_layer, n_batch, 2)),
                pltpu.SemaphoreType.DMA((2 * n_layer, n_batch // 2)),
                pltpu.SemaphoreType.DMA((2 * n_layer, n_batch, 2)),
                pltpu.SemaphoreType.DMA((2 * n_layer, n_batch // 2)),
                pltpu.SemaphoreType.DMA((2,)),
                pltpu.SemaphoreType.DMA((n_batch,)),
                pltpu.SemaphoreType.DMA((n_batch,)),
                pltpu.SemaphoreType.DMA((len(down_blocks(ch, 128)),)),
            ],
            compiler_params=pltpu.CompilerParams(collective_id=0, has_side_effects=True, vmem_limit_bytes=30 * 2**20),
        )(lat, time_emb, w_in, b_in, gn1_scale, gn1_shift, conv1_b, temb_b, gn2_scale, gn2_shift, conv2_b, temb_w, conv1_w, conv2_w, down_w, down_b)
        h0, h1, h2, d = pl.pallas_call(
            down_kernel,
            out_shape=(full, full, full, jax.ShapeDtypeStruct((n_batch, per, ch), BF16)),
            in_specs=[vmem],
            out_specs=(any_spec,) * 4,
            scratch_shapes=[
                pltpu.VMEM((3 * ch // 128, 1024, 128), BF16),
                pltpu.VMEM((3 * ch // 128, 1024, 128), BF16),
                pltpu.VMEM((6, cols + 16, 128), F32),
                pltpu.VMEM((n_batch, per, ch), BF16),
                pltpu.SemaphoreType.DMA((3, ch // 128)),
                pltpu.SemaphoreType.DMA,
            ],
            compiler_params=pltpu.CompilerParams(vmem_limit_bytes=12 * 2**20),
        )(hu)
        return tuple(v.reshape(n_batch, rows, cols, ch) for v in (h0, h1, h2)) + (d.reshape(n_batch, rows // 2, cols // 2, ch),)

    band_spec = P("dp", "sp", None, None)
    return jax.shard_map(band_program, mesh=mesh, in_specs=(band_spec, P("dp", None)) + (P(),) * 14, out_specs=(band_spec,) * 4, check_vma=False)
```

```python
import functools

import jax
import jax.numpy as jnp
from jax import lax
from jax.experimental import pallas as pl
from jax.experimental.pallas import tpu as pltpu
from jax.sharding import PartitionSpec as P

GN_GROUPS = 32
GN_EPS = 1e-5
MESH = pl.DeviceIdType.MESH
F32 = jnp.float32
BF16 = jnp.bfloat16
BUSY = 3


def exact_dot(rows, select):
    k = rows.shape[0]
    high = rows.astype(BF16).astype(F32)
    rest = rows - high
    mid = rest.astype(BF16).astype(F32)
    parts = [high, mid, rest - mid]
    if 3 * k < 16:
        parts.append(jnp.zeros((16 - 3 * k, rows.shape[1]), F32))
    out = jnp.dot(jnp.concatenate(parts, axis=0).astype(BF16), select, preferred_element_type=F32)
    return out[:k] + out[k:2 * k] + out[2 * k:3 * k]


def weight_copies(src, to_a, to_b, ch, last):
    n_a, lanes = to_a.shape[0], to_a.shape[-1]
    wide = n_a * lanes
    cps = [(src.at[:, :, :, pl.ds(k * lanes, lanes)], to_a.at[k]) for k in range(n_a)]
    cps.append((src.at[:, 1, :, pl.ds(wide, lanes)], to_b.at[0, :, pl.ds(0, ch)]))
    cps.append((src.at[:, 2, :, pl.ds(wide, lanes)], to_b.at[0, :, pl.ds(ch, ch)]))
    cps.append((src.at[:, 0, :, pl.ds(wide, lanes)], to_b.at[1, :, pl.ds(ch if last else 0, ch)]))
    return cps


def down_blocks(ch, lanes):
    wide = ch - lanes
    taps = [(dy, dx) for dy in range(3) for dx in range(3)]
    blocks = [(dy, dx, c) for c in range(0, wide, lanes) for dy, dx in taps]
    blocks += [(dy, dx, wide) for dy in range(3) for dx in (1, 2)]
    return blocks + [(dy, 0, wide) for dy in range(3)]


def block_at(hu, b, first, ch):
    n_tiles = hu.shape[1]
    return hu.at[first + b // (2 * n_tiles), b // 2 % n_tiles, pl.ds(b % 2 * ch, ch)]


def mix(a, b):
    both = [((k + 1) / (len(a) + 1), f) for k, f in enumerate(a)] + [((k + 1) / (len(b) + 1), f) for k, f in enumerate(b)]
    return [f for _, f in sorted(both, key=lambda t: t[0])]


def kernel(n, group, lat, temb, w_in, b_in, gn1_scale, gn1_shift, b1, temb_b, gn2_scale, gn2_shift, b2, temb_w, w1, w2, wd, down_b,
           hu, x0, x1, wa, wb, halo, gstat, lat_v, shift, in_w, vecs, emb, gather, spread, held, t_sem, w_sem, lat_sem, halo_sem, stat_sem, send_sem, stat_send, lat_send, edge_sem, edge_send, down_sem):
    n_tiles, n_pos, lanes = hu.shape[1:]
    n_batch = halo.shape[1]
    ch = n_tiles * lanes
    cols = halo.shape[4]
    rows = n_pos // cols
    n_layer = w1.shape[0]
    me = lax.axis_index("sp")
    nxt = lax.rem(me + 1, n)
    prv = lax.rem(me + n - 1, n)
    n_slots = wa.shape[0]
    wide = wa.shape[1] * lanes

    def wcopies(p):
        cps = weight_copies((w1, w2)[p % 2].at[p // 2], wa.at[p % wa.shape[0]], wb.at[p % wa.shape[0]], ch, False)
        return [pltpu.make_async_copy(a, b, w_sem.at[p, k]) for k, (a, b) in enumerate(cps)]

    lat_local = pltpu.make_async_copy(lat, lat_v.at[:, pl.ds(1, rows)], lat_sem.at[2])
    lat_local.start()
    t_rows = temb_w.shape[1]
    t_parts = [(l, lo, min(n_pos, t_rows - lo)) for l in range(n_layer) for lo in range(0, t_rows, n_pos)]

    def temb_slot(j):
        return (n_layer + 1) * n_batch + j

    temb_copies = [pltpu.make_async_copy(temb_w.at[l, pl.ds(lo, size), pl.ds(k * lanes, lanes)], hu.at[temb_slot(j), k, pl.ds(0, size)], t_sem.at[j, k]) for j, (l, lo, size) in enumerate(t_parts) for k in range(n_tiles)]
    for cp in temb_copies:
        cp.start()
    for cp in wcopies(0):
        cp.start()

    barrier = pltpu.get_barrier_semaphore()
    for k in range(1, n):
        pl.semaphore_signal(barrier, inc=1, device_id={"sp": lax.rem(me + k, n)}, device_id_type=MESH)
    lat_local.wait()
    pl.semaphore_wait(barrier, n - 1)

    lat_down = pltpu.make_async_remote_copy(lat_v.at[:, rows], lat_v.at[:, 0], lat_send.at[0], lat_sem.at[0], device_id={"sp": nxt}, device_id_type=MESH)
    lat_up = pltpu.make_async_remote_copy(lat_v.at[:, 1], lat_v.at[:, rows + 1], lat_send.at[1], lat_sem.at[1], device_id={"sp": prv}, device_id_type=MESH)
    lat_down.start()
    lat_up.start()
    for p in range(1, n_slots):
        for cp in wcopies(p):
            cp.start()
    for p in range(n_slots):
        wb[p, 1, :, pl.ds(ch, ch)] = jnp.zeros((3, ch, lanes), BF16)

    blank = jnp.zeros((4, ch), F32)
    in_w[...] = jnp.concatenate([w_in[dy, dx].astype(F32) if dx < 3 else blank for dy in range(3) for dx in range(4)], axis=0).astype(BF16)
    zrow = jnp.zeros((1, ch), F32)
    for p in range(2 * n_layer + 1):
        if p == 2 * n_layer:
            table = [zrow, zrow, zrow]
        else:
            refs = ((gn1_scale, gn1_shift, b1), (gn2_scale, gn2_shift, b2))[p % 2]
            table = [ref[pl.ds(p // 2, 1)].astype(F32) for ref in refs]
        vecs[p] = jnp.concatenate(table + [zrow] * 5, axis=0)
    lanes_of = lax.broadcasted_iota(jnp.int32, (ch, 128), 0) - group * lax.rem(lax.broadcasted_iota(jnp.int32, (ch, 128), 1), GN_GROUPS)
    gather[...] = jnp.where(jnp.logical_and(lanes_of >= 0, lanes_of < group), 1.0, 0.0).astype(BF16)
    lanes_of = lax.broadcasted_iota(jnp.int32, (128, ch), 1) - group * lax.rem(lax.broadcasted_iota(jnp.int32, (128, ch), 0), GN_GROUPS)
    spread[...] = jnp.where(jnp.logical_and(lanes_of >= 0, lanes_of < group), 1.0, 0.0).astype(BF16)
    for cp in temb_copies:
        cp.wait()
    z = temb[...].astype(F32) * 0.5
    act = (z + z * jnp.tanh(z)).astype(BF16)
    for p in range(2 * n_layer + 1):
        if p % 2:
            total = temb_b[pl.ds(p // 2, 1)].astype(F32)
            for j, (l, lo, size) in enumerate(t_parts):
                if l == p // 2:
                    part = jnp.concatenate([hu[temb_slot(j), k, pl.ds(0, size)] for k in range(n_tiles)], axis=1)
                    total = total + jnp.dot(act[:, lo:lo + size], part, preferred_element_type=F32)
            emb[p] = total
        else:
            emb[p] = jnp.zeros((n_batch, ch), F32)

    def weights_a(p):
        return jnp.concatenate([wa[lax.rem(p, n_slots), k].reshape(9 * ch, lanes) for k in range(wide // lanes)], axis=1)

    def weights_b(p):
        return jnp.concatenate([wb[lax.rem(p, n_slots), k].reshape(6 * ch, lanes) for k in range(2)], axis=1)

    def source(p):
        odd = lax.rem(p, 2)
        return ((1 - odd) * (p // 2) + odd * (n_layer + 1)) * n_batch

    def edge_down(s):
        return pltpu.make_async_remote_copy(hu.at[n_layer * n_batch + s, :, pl.ds(n_pos - cols, cols)], hu.at[(n_layer + 2) * n_batch, :, pl.ds(s * cols, cols)], edge_send.at[s], edge_sem.at[s], device_id={"sp": nxt}, device_id_type=MESH)

    def halo_down(p, s):
        buf = source(p)
        return pltpu.make_async_remote_copy(hu.at[buf + s, :, pl.ds(n_pos - cols, cols)], halo.at[p, s, 0], send_sem.at[p, s, 0], halo_sem.at[p, s, 0], device_id={"sp": nxt}, device_id_type=MESH)

    def halo_up(p, s):
        buf = source(p)
        return pltpu.make_async_remote_copy(hu.at[buf + s, :, pl.ds(0, cols)], halo.at[p, s, 1], send_sem.at[p, s, 1], halo_sem.at[p, s, 1], device_id={"sp": prv}, device_id_type=MESH)

    def stat_copy(p, i, k):
        return pltpu.make_async_remote_copy(gstat.at[p, i, 0], gstat.at[p, i, k], stat_send.at[p, i], stat_sem.at[p, i], device_id={"sp": lax.rem(me + k, n)}, device_id_type=MESH)

    def stat_all(p, i):
        return pltpu.make_async_remote_copy(gstat.at[p, i, pl.ds(1, n - 1)], gstat.at[p, i, pl.ds(1, n - 1)], stat_send.at[p, i], stat_sem.at[p, i], device_id={"sp": nxt}, device_id_type=MESH)

    def send_stats(p, i):
        for k in range(1, n):
            stat_copy(p, i, k).start()

    def send_rows(p, i):
        for s in (2 * i, 2 * i + 1):
            halo_down(p, s).start()
            halo_up(p, s).start()

    own_lanes = lax.broadcasted_iota(jnp.int32, (4, 128), 1) - GN_GROUPS * lax.broadcasted_iota(jnp.int32, (4, 128), 0)
    own_lanes = jnp.logical_and(own_lanes >= 0, own_lanes < GN_GROUPS)

    def keep_sums(q, sums):
        held[q] = jnp.concatenate(sums + [jnp.zeros((4, ch), F32)], axis=0)

    def put_stats(p, i, q):
        tot = exact_dot(held[q][:4], gather[...])
        gstat[p, i, 0] = jnp.sum(jnp.where(own_lanes, tot, 0.0), axis=0, keepdims=True)

    def arrive_rows(p, s):
        halo_down(p, s).wait_recv()
        halo_up(p, s).wait_recv()

    def coefficients(p, s, which):
        tot = jnp.sum(gstat[p, s // 2], axis=0)
        pick = own_lanes[2 * which:2 * which + 2]
        tot = exact_dot(jnp.where(pick, tot, 0.0), spread[...])
        count = float(n * n_pos * group)
        mean = tot[0:1] / count
        var = tot[1:2] / count - mean * mean
        v = vecs[p]
        scale = lax.rsqrt(var + GN_EPS) * v[0:1]
        offset = v[1:2] - mean * scale + emb[p, pl.ds(s, 1)] * scale
        return scale * 0.5, offset * 0.5

    pad = 8
    shift[...] = jnp.zeros_like(shift)

    def norm_piece(p, s, r, k, scale, offset, x):
        scale, offset = scale[:, k * 128:(k + 1) * 128], offset[:, k * 128:(k + 1) * 128]
        if r == 0:
            src = halo[p, s, 0, k]
            keep = (me > 0).astype(F32)
            scale, offset = scale * keep, offset * keep
        elif r == rows + 1:
            src = halo[p, s, 1, k]
            keep = (me < n - 1).astype(F32)
            scale, offset = scale * keep, offset * keep
        else:
            src = hu[source(p) + s, k, pl.ds((r - 1) * cols, cols)]
        z = src.astype(F32) * scale + offset
        y = z + z * jnp.tanh(z)
        at = pl.ds(r * cols, cols)
        slot = (r * n_tiles + k) % shift.shape[0]
        shift[slot, pl.ds(pad, cols)] = y
        x[n_tiles + k, at] = y.astype(BF16)
        x[k, at] = shift[slot, pl.ds(pad - 1, cols)].astype(BF16)
        x[2 * n_tiles + k, at] = shift[slot, pl.ds(pad + 1, cols)].astype(BF16)

    def norm_work(p, s, which, x):
        coef = []

        def first():
            coef.extend(coefficients(p, s, which))

        def piece(r, k):
            return lambda: norm_piece(p, s, r, k, coef[0], coef[1], x)

        return [first] + [piece(r, k) for r in range(rows + 2) for k in range(ch // 128)]

    def conv_sample(p, s, x, side, sizes):
        odd = lax.rem(p, 2)
        bias = vecs[p, 2:3]
        e_next = emb[p + 1, pl.ds(s, 1)]
        tail = ch - wide
        col0 = lax.broadcasted_iota(jnp.int32, (cols, tail), 0) == 0
        sums_a = [(jnp.zeros((8, wide), F32),) * 2]
        sums_b = [(jnp.zeros((8, tail), F32),) * 2]

        def finish(at, lo, width, raw, sums):
            parts = []
            for k in range(lo // 128, (lo + width) // 128):
                piece = slice(k * 128, (k + 1) * 128)
                out = (raw[:, k * 128 - lo:(k + 1) * 128 - lo] + bias[:, piece]).astype(BF16).astype(F32)
                old = hu[p // 2 * n_batch + s, k, at].astype(F32)
                new = (jnp.where(odd == 1, old, 0.0) + out).astype(BF16)
                hu[source(p + 1) + s, k, at] = new
                v = new.astype(F32) + e_next[:, piece]
                v = v.reshape(v.shape[0] // 8, 8, 128)
                parts.append((jnp.sum(v, axis=0), jnp.sum(v * v, axis=0)))
            sums[0] = tuple(old + jnp.concatenate([q[j] for q in parts], axis=1) for j, old in enumerate(sums[0]))

        def end_a(m, j, a):
            return lambda: finish(pl.ds(m + j * cols, cols), 0, wide, a[j * cols:(j + 1) * cols], sums_a)

        def end_b(m, j, b):
            def work():
                part = b[j * cols:(j + 1) * cols]
                raw = part[:, :tail] + jnp.where(col0, 0.0, pltpu.roll(part[:, tail:], 1, axis=0))
                finish(pl.ds(m + j * cols, cols), wide, tail, raw, sums_b)
            return work

        starts = [sum(sizes[:j]) for j in range(len(sizes))]
        side = list(side)
        share = -(-len(side) // BUSY)
        pending = []
        for m, size in zip(starts, sizes):
            for kind in range(2):
                lo = ch if kind else 0
                lhs = jnp.concatenate([x[k, pl.ds(m + dy * cols, size)] for dy in range(3) for k in range(lo // 128, 3 * n_tiles)], axis=1)
                w = weights_b(p) if kind else weights_a(p)
                out = jnp.dot(lhs, w, preferred_element_type=F32)
                now, side = side[:share], side[share:]
                for f in mix(pending, now):
                    f()
                pending = [(end_b if kind else end_a)(m, j, out) for j in range(size // cols)]
        for f in pending:
            f()
        return [jnp.concatenate([jnp.sum(sa, axis=0, keepdims=True), jnp.sum(sb, axis=0, keepdims=True)], axis=1) for sa, sb in zip(sums_a[0], sums_b[0])]

    lat_down.wait_recv()
    lat_up.wait_recv()

    half = n_batch // 2

    def conv_in(s):
        tiles = []
        for r in range(rows + 2):
            t = lat_v[s, r]
            if r == 0:
                t = jnp.where(me > 0, t, jnp.zeros_like(t))
            if r == rows + 1:
                t = jnp.where(me < n - 1, t, jnp.zeros_like(t))
            tiles.append(t)
        lhs = jnp.concatenate([jnp.concatenate(tiles[r:r + 3], axis=0) for r in range(rows)], axis=1)
        out = lax.dot_general(lhs, in_w[...], (((0,), (0,)), ((), ())), preferred_element_type=F32)
        new = (out + b_in[...].astype(F32).reshape(1, ch)).astype(BF16)
        for k in range(n_tiles):
            hu[s, k] = new[:, k * 128:(k + 1) * 128]
        v = new.astype(F32)
        return [jnp.sum(v, axis=0, keepdims=True), jnp.sum(v * v, axis=0, keepdims=True)]

    def conv_in_step(i, carry):
        @pl.when(i > 0)
        def _():
            send_stats(0, i - 1)
            send_rows(0, i - 1)

        keep_sums(i // (half - 1), conv_in(2 * i) + conv_in(2 * i + 1))
        put_stats(0, i, 0)
        return carry

    lax.fori_loop(0, half, conv_in_step, 0)
    send_rows(0, half - 1)
    stat_all(0, 0).wait_recv()
    arrive_rows(0, 0)
    for f in norm_work(0, 0, 0, x0):
        f()


    spare = (n_layer + 1) * n_batch
    down_list = down_blocks(ch, lanes)
    n_lent = len(down_list) // (2 * n_tiles) + 1
    down_copies = [pltpu.make_async_copy(wd.at[dy, dx, :, pl.ds(c, lanes)], block_at(hu, b, spare, ch), down_sem.at[b]) for b, (dy, dx, c) in enumerate(down_list)]

    def step(t, carry):
        p, i = t // half, lax.rem(t, half)
        s0, s1 = 2 * i, 2 * i + 1
        after = lax.rem(t + 1, half * 2 * n_layer)
        pn, sn = after // half, 2 * lax.rem(after, half)
        pb, ib = (t + half - 1) // half - 1, lax.rem(t + half - 1, half)
        ps, js = (t + half - 2) // half - 1, lax.rem(t + half - 2, half)
        arrive_rows(p, s1)

        @pl.when(t + 1 < half * 2 * n_layer)
        def _():
            stat_all(pn, sn // 2).wait_recv()
            arrive_rows(pn, sn)

        for q in range(2 * n_layer):
            @pl.when(jnp.logical_and(p == q, i == 0))
            def _():
                for cp in wcopies(q):
                    cp.wait()

        @pl.when(t == half * 2 * n_layer - 1)
        def _():
            for s in range(n_lent):
                halo_down(2 * n_layer - 1, s).wait_send()
                halo_up(2 * n_layer - 1, s).wait_send()
            for cp in down_copies:
                cp.start()

        for q in range(n_slots, 2 * n_layer):
            @pl.when(jnp.logical_and(p == q - n_slots + 1, i == 0))
            def _():
                for cp in wcopies(q):
                    cp.start()

        @pl.when(p > 0)
        def _():
            for s in (s0, s1):
                halo_down(p - 1, s).wait_send()
                halo_up(p - 1, s).wait_send()

        @pl.when(jnp.logical_and(t > 0, pb < 2 * n_layer - 1))
        def _():
            send_rows(pb + 1, ib)

        @pl.when(jnp.logical_and(t > 0, pb == 2 * n_layer - 1))
        def _():
            for j in range(2):
                edge_down(2 * ib + j).start()

        @pl.when(jnp.logical_and(t > 0, ps < 2 * n_layer - 1))
        def _():
            send_stats(ps + 1, js)

        old, new = lax.rem(t + 1, 2), lax.rem(t, 2)
        sums = conv_sample(p, s0, x0, [lambda: put_stats(pb + 1, ib, old)] + norm_work(p, s1, 1, x1), [n_pos // 2, n_pos // 2])
        sums = sums + conv_sample(p, s1, x1, norm_work(pn, sn, 0, x0), [n_pos // 2, n_pos // 4, n_pos // 4])
        keep_sums(new, sums)
        return carry

    lax.fori_loop(0, half * 2 * n_layer, step, 0)
    for j in range(2):
        edge_down(n_batch - 2 + j).start()
    bias_slot = spare + len(down_list) // (2 * n_tiles)
    bias_row = down_b[...].astype(F32).reshape(1, ch)
    for k in range(n_tiles):
        hu[bias_slot, k, pl.ds(n_pos - 16, 16)] = jnp.broadcast_to(bias_row[:, k * lanes:(k + 1) * lanes], (16, lanes)).astype(BF16)
    for cp in down_copies:
        cp.wait()

    def drain_stats(t, carry):
        stat_all(t // half, lax.rem(t, half)).wait_send()
        return carry

    lax.fori_loop(0, 2 * n_layer * half, drain_stats, 0)

    def drain_rows(s, carry):
        edge_down(s).wait()
        return carry

    for s in range(n_lent, n_batch):
        halo_down(2 * n_layer - 1, s).wait_send()
        halo_up(2 * n_layer - 1, s).wait_send()

    lax.fori_loop(0, n_batch, drain_rows, 0)
    lat_down.wait_send()
    lat_up.wait_send()


def down_kernel(hu, h0_out, h1_out, h2_out, d_out, x0, x1, shift, dn_out, out_sem, d_sem):
    n_tiles, n_pos, lanes = hu.shape[1:]
    n_batch, per, ch = d_out.shape
    cols = n_pos // n_batch
    rows = n_pos // cols
    me = lax.axis_index("sp")
    half = n_batch // 2
    pad = 8
    wide = ch - lanes
    spare = 3 * n_batch
    n_blocks = len(down_blocks(ch, lanes))
    blocks = [block_at(hu, b, spare, ch) for b in range(n_blocks)]
    outs = [pltpu.make_async_copy(hu.at[pl.ds(q * n_batch, n_batch), k], out.at[:, :, pl.ds(k * lanes, lanes)], out_sem.at[q, k]) for q, out in enumerate((h0_out, h1_out, h2_out)) for k in range(n_tiles)]
    for cp in outs:
        cp.start()
    shift[...] = jnp.zeros_like(shift)
    wide_out = cols // 2
    dn_rows = rows // 2
    per = dn_rows * wide_out

    def down_prep(s, base):
        for r in range(rows + 1):
            for k in range(n_tiles):
                if r == 0:
                    src = hu[hu.shape[0] - 1, k, pl.ds(s * cols, cols)].astype(F32) * (me > 0).astype(F32)
                else:
                    src = hu[2 * n_batch + s, k, pl.ds((r - 1) * cols, cols)].astype(F32)
                slot = (r * n_tiles + k) % shift.shape[0]
                shift[slot, pl.ds(pad, cols)] = src
                at = pl.ds(base + (r // 2) * wide_out, wide_out)
                x = x1 if r % 2 else x0
                for j in range(3):
                    x[j * n_tiles + k, at] = shift[slot, pl.ds(pad - 1 + j, wide_out, stride=2)].astype(BF16)

    def put_pair(i):
        return pltpu.make_async_copy(dn_out.at[pl.ds(2 * i, 2)], d_out.at[pl.ds(2 * i, 2)], d_sem)

    def down_step(i, carry):
        @pl.when(i > 0)
        def _():
            put_pair(i - 1).start()

        stride = 512
        for j in range(2):
            down_prep(2 * i + j, j * stride)

        rest = 9 * (n_tiles - 1)
        w_a = jnp.concatenate([jnp.concatenate([blocks[c * 9 + k][...] for k in range(9)], axis=0) for c in range(n_tiles - 1)], axis=1)
        none = jnp.zeros((ch, lanes), BF16)
        w_here = jnp.concatenate([blocks[rest + k][...] for k in range(6)], axis=0)
        w_before = jnp.concatenate([v for k in range(3) for v in (none, blocks[rest + 6 + k][...])], axis=0)
        w_b = jnp.concatenate([w_here, w_before], axis=1)
        def lhs(lo):
            parts = []
            for x, off in ((x0, 0), (x1, 0), (x0, wide_out)):
                for k in range(lo // 128, 3 * n_tiles):
                    parts.append(jnp.concatenate([x[k, pl.ds(j * stride + off, per)] for j in range(2)], axis=0))
            return jnp.concatenate(parts, axis=1)

        bias = jnp.concatenate([hu[spare + n_blocks // (2 * n_tiles), k, pl.ds(n_pos - 16, 16)].astype(F32)[:1] for k in range(n_tiles)], axis=1)
        tail = ch - wide
        a = jnp.dot(lhs(0), w_a, preferred_element_type=F32)
        b = jnp.dot(lhs(ch), w_b, preferred_element_type=F32)
        edge = lax.rem(lax.broadcasted_iota(jnp.int32, (2 * per, tail), 0), wide_out) == 0
        b = b[:, :tail] + jnp.where(edge, 0.0, pltpu.roll(b[:, tail:], 1, axis=0))
        for j in range(2):
            dn_out[2 * i + j, :, pl.ds(0, wide)] = (a[j * per:(j + 1) * per] + bias[:, :wide]).astype(BF16)
            dn_out[2 * i + j, :, pl.ds(wide, tail)] = (b[j * per:(j + 1) * per] + bias[:, wide:]).astype(BF16)
        return carry

    lax.fori_loop(0, half, down_step, 0)
    put_pair(half - 1).start()
    for cp in outs:
        cp.wait()
    pltpu.make_async_copy(dn_out, d_out, d_sem).wait()


def solution(mesh):
    n = mesh.shape["sp"]

    def band_program(latent, time_emb, w_in, b_in, gn1_scale, gn1_shift, conv1_w, conv1_b, temb_w, temb_b, gn2_scale, gn2_shift, conv2_w, conv2_b, down_w, down_b):
        n_batch, rows, cols, lat_ch = latent.shape
        n_layer, ch = conv1_b.shape
        n_pos = rows * cols
        group = ch // GN_GROUPS
        wide = 256
        lt = jnp.transpose(latent, (0, 1, 3, 2))
        lp = jnp.pad(lt, ((0, 0), (0, 0), (0, 0), (1, 1)))
        shifted = [lp[..., k:k + cols] for k in range(3)]
        pad_rows = 16 - 3 * lat_ch
        lat = jnp.concatenate(shifted + [jnp.zeros((n_batch, rows, pad_rows, cols), BF16)], axis=2)
        any_spec = pl.BlockSpec(memory_space=pltpu.HBM)
        vmem = pl.BlockSpec(memory_space=pltpu.VMEM)
        full = jax.ShapeDtypeStruct((n_batch, n_pos, ch), BF16)
        per = n_pos // 4
        hu = pl.pallas_call(
            functools.partial(kernel, n, group),
            out_shape=pltpu.VMEM(((n_layer + 2) * n_batch + 1, ch // 128, n_pos, 128), BF16),
            in_specs=[any_spec] + [vmem] * 10 + [any_spec] * 4 + [vmem],
            out_specs=vmem,
            scratch_shapes=[
                pltpu.VMEM((3 * ch // 128, (rows + 2) * cols, 128), BF16),
                pltpu.VMEM((3 * ch // 128, (rows + 2) * cols, 128), BF16),
                pltpu.VMEM((3, wide // 128, 3, 3, ch, 128), BF16),
                pltpu.VMEM((3, 2, 3, 2 * ch, 128), BF16),
                pltpu.VMEM((2 * n_layer, n_batch, 2, ch // 128, cols, 128), BF16),
                pltpu.VMEM((2 * n_layer + 1, n_batch // 2, n, 1, 128), F32),
                pltpu.VMEM((n_batch, rows + 2, 16, cols), BF16),
                pltpu.VMEM((6, cols + 16, 128), F32),
                pltpu.VMEM((48, ch), BF16),
                pltpu.VMEM((2 * n_layer + 1, 8, ch), F32),
                pltpu.VMEM((2 * n_layer + 1, n_batch, ch), F32),
                pltpu.VMEM((ch, 128), BF16),
                pltpu.VMEM((128, ch), BF16),
                pltpu.VMEM((2, 8, ch), F32),
                pltpu.SemaphoreType.DMA((8, ch // 128)),
                pltpu.SemaphoreType.DMA((2 * n_layer, 5)),
                pltpu.SemaphoreType.DMA((3,)),
                pltpu.SemaphoreType.DMA((2 * n_layer, n_batch, 2)),
                pltpu.SemaphoreType.DMA((2 * n_layer, n_batch // 2)),
                pltpu.SemaphoreType.DMA((2 * n_layer, n_batch, 2)),
                pltpu.SemaphoreType.DMA((2 * n_layer, n_batch // 2)),
                pltpu.SemaphoreType.DMA((2,)),
                pltpu.SemaphoreType.DMA((n_batch,)),
                pltpu.SemaphoreType.DMA((n_batch,)),
                pltpu.SemaphoreType.DMA((len(down_blocks(ch, 128)),)),
            ],
            compiler_params=pltpu.CompilerParams(collective_id=0, has_side_effects=True, vmem_limit_bytes=30 * 2**20),
        )(lat, time_emb, w_in, b_in, gn1_scale, gn1_shift, conv1_b, temb_b, gn2_scale, gn2_shift, conv2_b, temb_w, conv1_w, conv2_w, down_w, down_b)
        h0, h1, h2, d = pl.pallas_call(
            down_kernel,
            out_shape=(full, full, full, jax.ShapeDtypeStruct((n_batch, per, ch), BF16)),
            in_specs=[vmem],
            out_specs=(any_spec,) * 4,
            scratch_shapes=[
                pltpu.VMEM((3 * ch // 128, 1024, 128), BF16),
                pltpu.VMEM((3 * ch // 128, 1024, 128), BF16),
                pltpu.VMEM((6, cols + 16, 128), F32),
                pltpu.VMEM((n_batch, per, ch), BF16),
                pltpu.SemaphoreType.DMA((3, ch // 128)),
                pltpu.SemaphoreType.DMA,
            ],
            compiler_params=pltpu.CompilerParams(vmem_limit_bytes=12 * 2**20),
        )(hu)
        return tuple(v.reshape(n_batch, rows, cols, ch) for v in (h0, h1, h2)) + (d.reshape(n_batch, rows // 2, cols // 2, ch),)

    band_spec = P("dp", "sp", None, None)
    return jax.shard_map(band_program, mesh=mesh, in_specs=(band_spec, P("dp", None)) + (P(),) * 14, out_specs=(band_spec,) * 4, check_vma=False)
```
